32 devices in a mesh: orb: 8 (over z, y), clu: 4 (over x, core).
Axes of the slice: x: 2, y: 2, z: 4, core: 2. Of those that a mesh axis runs over, the one named last changes fastest.
Arguments:
- integrals: bfloat16 [1024, 1024, 512], P('orb', 'clu'), may hold values from -1.1953125 to 1.1953125
- metric: bfloat16 [1024, 1024], P(None, 'orb'), may hold values from -0.1875 to 0.1875
- occ_energy: float32 [1024], replicated, may hold values from -2 to -0.5
- virt_energy: float32 [512], replicated, may hold values from 0.5 to 4
- orbital_order: int32 [4, 256], replicated, may hold values from 0 to 255, each once within a row
- pair_first: int32 [4, 8, 4], P('clu', 'orb'), may hold values from 0 to 31
- pair_second: int32 [4, 8, 4], replicated, may hold values from 0 to 255
- pair_live: int32 [4, 8, 4], P('clu', 'orb'), may hold values 0 or 1
Outputs:
- gamma: bfloat16 [1024, 1024, 512], P('orb', 'clu')
The draws below stay inside these ranges and needn't reach their ends.
Inputs may be any that keep to these rules, and one draw needn't show every extreme that they name: `orbital_order`: each row is a permutation of 0 to 255. `pair_second`: slot s names an orbital of cluster s.
All inputs are finite; a program needn't handle non-finite values. No bound on the sum of `pair_live` on one device may be relied on, other than what follows from the above.
Results may differ from the reference program's by a relative error of at most 0.0052.
Values may be sent and summed in bfloat16 or wider, within the bound.
A program may use at most 256 MiB of HBM per device.

```python
import math
import jax
import jax.numpy as jnp
import numpy as np
from jax import lax

X = 1024
OCC = 256
V = 512
PER_CLU = 1
ORBITALS = 1024
OD = 32
PAIRS = 4
N_ORB = 8
N_CLU = 4


def set_ends(result, key, smallest, top_value):
    spot = [jax.random.randint(jax.random.fold_in(key, axis), (), 0, length) for axis, length in enumerate(result.shape)]
    longest = result.shape.index(max(result.shape))
    next_to = spot[:longest] + [(spot[longest] + 1) % result.shape[longest]] + spot[longest + 1:]
    return result.at[tuple(spot)].set(smallest).at[tuple(next_to)].set(top_value)


def block_levels(own_key, extent, shards, least, high):
    factor_of = 1.0
    for position, parts in shards:
        steps = jax.random.uniform(jax.random.fold_in(jax.random.fold_in(own_key, 6), position), (parts,), jnp.float32, least / len(shards), high / len(shards))
        factor_of = factor_of * jnp.repeat(jnp.exp(steps), extent[position] // parts).reshape((-1,) + (1,) * (len(extent) - 1 - position))
    return factor_of


def rank_bounds(count, skew):
    portions = [(1 << 20) // math.isqrt(standing ** skew) + 1 for standing in range(1, count + 1)]
    scale = 1 + sum(portions) // (1 << 30)
    return np.cumsum(np.array([max(1, weight // scale) for weight in portions]))


def skewed_ids(stream_key, dims, amount, slope):
    listing = rank_bounds(amount, slope)
    ticket = jax.random.randint(jax.random.fold_in(stream_key, 1), dims, 0, int(listing[amount - 1]))
    grade = jnp.searchsorted(jnp.asarray(listing, jnp.int32), ticket, side="right")
    return jax.random.permutation(jax.random.fold_in(stream_key, 2), amount)[grade].astype(jnp.int32)


def scatter_about(rng, dims, deviation, limit, split=(), held_as=jnp.bfloat16):
    array = jax.random.normal(rng, dims, jnp.float32) * deviation
    if len(split) > 0:
        array = block_levels(rng, dims, split, -0.22, 0.18) * array
    return jnp.clip(array, min=-limit, max=limit).astype(held_as)


def setup_inputs(seed: int = 0) -> dict:
    keys = jax.random.split(jax.random.key(seed), 9)
    integrals = scatter_about(keys[0], (X, ORBITALS, V), 0.2, 1.1953125, ((0, 8), (1, 4)))
    metric = scatter_about(keys[1], (X, X), X ** -0.5, 0.1875, ((1, 8),))
    occ_energy = jnp.clip(jax.random.uniform(keys[2], (ORBITALS,), jnp.float32, -2.0, -0.5), -2.0, -0.5)
    virt_energy = jnp.clip(jax.random.uniform(keys[3], (V,), jnp.float32, 0.5, 4.0), 0.5, 4.0)
    orbital_order = jax.vmap(lambda own: jax.random.permutation(own, OCC))(jax.random.split(keys[4], N_CLU)).reshape((N_CLU, OCC)).astype(jnp.int32)
    pair_first = set_ends(jax.random.randint(keys[5], (N_CLU, N_ORB, PAIRS), 0, OD), jax.random.fold_in(keys[5], 1), 0, OD - 1).astype(jnp.int32)
    pair_second = set_ends(skewed_ids(keys[6], (N_CLU, N_ORB, PAIRS), OCC, 2), jax.random.fold_in(keys[6], 3), 0, OCC - 1).astype(jnp.int32)
    pair_live = set_ends((jax.random.randint(keys[7], (N_CLU, N_ORB, PAIRS), 0, 4) < 3).astype(jnp.int32), jax.random.fold_in(keys[7], 1), 0, 1)
    return dict(integrals=integrals, metric=metric, occ_energy=occ_energy, virt_energy=virt_energy, orbital_order=orbital_order, pair_first=pair_first, pair_second=pair_second, pair_live=pair_live)


def reference(integrals, metric, occ_energy, virt_energy, orbital_order, pair_first, pair_second, pair_live):
    owned_count = OCC // N_ORB
    fitted_blocks = []
    for cluster in range(N_CLU):
        cluster_rows = integrals[:, cluster * OCC:(cluster + 1) * OCC, :].reshape(X, OCC * V)
        product = jnp.dot(metric.T, cluster_rows, preferred_element_type=jnp.float32)
        fitted_blocks.append(product.astype(jnp.bfloat16).reshape(X, OCC, V))
    fitted = jnp.concatenate(fitted_blocks, axis=1)
    slot_cluster = (jnp.arange(PAIRS, dtype=jnp.int32) // PER_CLU).astype(jnp.int32)

    def device_gamma(device_index):
        cluster = device_index // N_ORB
        orb_column = device_index % N_ORB
        order_row = orbital_order[cluster]
        owned_orbs = lax.dynamic_slice_in_dim(order_row, orb_column * owned_count, owned_count) + cluster * OCC
        first_slot = pair_first[cluster, orb_column]
        second_orb = pair_second[cluster, orb_column] + slot_cluster * OCC
        live_mask = pair_live[cluster, orb_column].astype(jnp.float32)
        first_orb = jnp.take(owned_orbs, first_slot)
        first_fit = jnp.take(fitted, first_orb, axis=1).astype(jnp.float32)
        second_fit = jnp.take(fitted, second_orb, axis=1).astype(jnp.float32)
        intersection = jnp.einsum("xpa,xpb->pab", first_fit, second_fit)
        denominator = (virt_energy[None, :, None] + virt_energy[None, None, :]
                       - occ_energy[first_orb][:, None, None] - occ_energy[second_orb][:, None, None])
        amplitude = (live_mask[:, None, None] * intersection / denominator).astype(jnp.bfloat16).astype(jnp.float32)
        contribution = jnp.einsum("pab,xpb->xpa", amplitude, second_fit)
        onehot = (first_slot[:, None] == jnp.arange(owned_count, dtype=jnp.int32)[None, :]).astype(jnp.float32)
        gamma_local = jnp.einsum("xpa,pd->xda", contribution, onehot, precision=lax.Precision.HIGHEST)
        return gamma_local.astype(jnp.bfloat16)

    per_device = lax.map(device_gamma, jnp.arange(N_CLU * N_ORB, dtype=jnp.int32))
    per_device = per_device.reshape(N_CLU, N_ORB, X, owned_count, V)
    cluster_gammas = []
    for cluster in range(N_CLU):
        ordered = jnp.transpose(per_device[cluster], (1, 0, 2, 3)).reshape(X, OCC, V)
        inverse = jnp.argsort(orbital_order[cluster]).astype(jnp.int32)
        cluster_gammas.append(jnp.take(ordered, inverse, axis=1))
    return jnp.concatenate(cluster_gammas, axis=1)
```

```python
import functools

import jax
import jax.numpy as jnp
from jax import lax
from jax.experimental import pallas as pl
from jax.experimental.pallas import tpu as pltpu
from jax.sharding import PartitionSpec as P

MESH = pl.DeviceIdType.MESH


def enter(orb, clu):
    barrier = pltpu.get_barrier_semaphore()
    d, c = lax.axis_index("orb"), lax.axis_index("clu")
    me = d * clu + c

    def greet(k, carry):
        to = lax.rem(me + k, orb * clu)
        pl.semaphore_signal(barrier, inc=1, device_id=(to // clu, lax.rem(to, clu)), device_id_type=MESH)
        return carry

    lax.fori_loop(1, orb * clu, greet, 0)
    pl.semaphore_wait(barrier, orb * clu - 1)


def gather_kernel(orb, clu, slots, per, xs, first_ref, second_ref, metric_ref, rows_ref, full_ref,
                  fs, fr, ss, sr, ms, mr, local):
    d, c = lax.axis_index("orb"), lax.axis_index("clu")
    me = d * clu + c
    enter(orb, clu)
    mine = pl.ds(pl.multiple_of(d * xs, xs), xs)

    def first_copy(to, at, sem):
        return pltpu.make_async_remote_copy(
            first_ref.at[to], rows_ref.at[pl.ds(0, slots), at], fs.at[to], fr.at[sem],
            device_id=(to, c), device_id_type=MESH)

    def metric_copy(to, sem):
        return pltpu.make_async_remote_copy(
            metric_ref, full_ref.at[sem], ms.at[to], mr.at[sem], device_id=(to, c), device_id_type=MESH)

    def second_copy(to, at, cluster, sem):
        return pltpu.make_async_remote_copy(
            second_ref.at[to], rows_ref.at[pl.ds(slots + cluster * per, per), at], ss.at[to], sr.at[sem],
            device_id=(to // clu, lax.rem(to, clu)), device_id_type=MESH)

    own = [
        pltpu.make_async_copy(first_ref.at[d], rows_ref.at[pl.ds(0, slots), mine], local.at[0]),
        pltpu.make_async_copy(second_ref.at[me], rows_ref.at[pl.ds(slots + c * per, per), mine], local.at[1]),
        pltpu.make_async_copy(metric_ref, full_ref.at[d], local.at[2]),
    ]
    for copy in own:
        copy.start()

    def start_orb(k, carry):
        to = lax.rem(d + k, orb)
        metric_copy(to, d).start()
        first_copy(to, mine, d).start()
        return carry

    def start_all(k, carry):
        to = lax.rem(me + k, orb * clu)
        second_copy(to, mine, c, me).start()
        return carry

    lax.fori_loop(1, orb, start_orb, 0)
    lax.fori_loop(1, orb * clu, start_all, 0)

    def end_orb(k, carry):
        to = lax.rem(d + k, orb)
        at = pl.ds(pl.multiple_of(to * xs, xs), xs)
        metric_copy(to, to).wait()
        first_copy(to, at, to).wait()
        return carry

    def end_all(k, carry):
        to = lax.rem(me + k, orb * clu)
        at = pl.ds(pl.multiple_of(to // clu * xs, xs), xs)
        second_copy(to, at, lax.rem(to, clu), to).wait()
        return carry

    lax.fori_loop(1, orb, end_orb, 0)
    lax.fori_loop(1, orb * clu, end_all, 0)
    for copy in own:
        copy.wait()


def return_kernel(orb, clu, xs, gamma_ref, back_ref, send, recv, local):
    d, c = lax.axis_index("orb"), lax.axis_index("clu")
    enter(orb, clu)

    def copy_to(to, sem):
        return pltpu.make_async_remote_copy(
            gamma_ref.at[:, pl.ds(pl.multiple_of(to * xs, xs), xs)], back_ref.at[sem], send.at[to], recv.at[sem],
            device_id=(to, c), device_id_type=MESH)

    own = pltpu.make_async_copy(
        gamma_ref.at[:, pl.ds(pl.multiple_of(d * xs, xs), xs)], back_ref.at[d], local.at[0])
    own.start()

    def start(k, carry):
        copy_to(lax.rem(d + k, orb), d).start()
        return carry

    def end(k, carry):
        to = lax.rem(d + k, orb)
        copy_to(to, to).wait()
        return carry

    lax.fori_loop(1, orb, start, 0)
    lax.fori_loop(1, orb, end, 0)
    own.wait()


def on_device(
    integrals, metric, occ_energy, virt_energy, orbital_order, pair_first, pair_second, pair_live
):
    orb, clu = lax.axis_size("orb"), lax.axis_size("clu")
    d, c = lax.axis_index("orb"), lax.axis_index("clu")
    xs, occ, virt = integrals.shape
    aux = metric.shape[0]
    owned = occ // orb
    slots = pair_second.shape[2]
    per = slots // clu
    any_space = pl.BlockSpec(memory_space=pl.ANY)
    dma = pltpu.SemaphoreType.DMA

    own_order = lax.dynamic_index_in_dim(orbital_order, c, 0, keepdims=False)
    all_first = lax.all_gather(pair_first[0, 0], "orb", axis=0, tiled=False)
    first_in = jnp.take_along_axis(own_order.reshape(orb, owned), all_first, axis=1)
    wanted = lax.dynamic_slice_in_dim(pair_second, c * per, per, 2).transpose(1, 0, 2)
    index = jnp.concatenate([first_in.reshape(-1), wanted.reshape(-1)])
    pick = (index[:, None] == jnp.arange(occ, dtype=jnp.int32)[None, :]).astype(jnp.bfloat16)
    picked = jnp.einsum("jo,poa->pja", pick, integrals).transpose(1, 0, 2)
    first_rows = picked[: orb * slots].reshape(orb, slots, xs, virt)
    second_rows = picked[orb * slots :].reshape(orb * clu, per, xs, virt)

    rows, full = pl.pallas_call(
        functools.partial(gather_kernel, orb, clu, slots, per, xs),
        out_shape=[
            jax.ShapeDtypeStruct((2 * slots, aux, virt), jnp.bfloat16),
            jax.ShapeDtypeStruct((orb,) + metric.shape, jnp.bfloat16),
        ],
        in_specs=[any_space] * 3,
        out_specs=[any_space] * 2,
        scratch_shapes=[dma((orb,)), dma((orb,)), dma((orb * clu,)), dma((orb * clu,)), dma((orb,)), dma((orb,)), dma((3,))],
        compiler_params=pltpu.CompilerParams(collective_id=0, has_side_effects=True),
    )(first_rows, second_rows, metric)

    whole_metric = full.transpose(0, 2, 1).reshape(aux, aux)
    fitted = jnp.einsum("qp,spa->sqa", whole_metric, rows, preferred_element_type=jnp.float32).astype(jnp.bfloat16)
    first_fit, second_fit = fitted[:slots], fitted[slots:]
    intersection = jnp.einsum("sqa,sqb->sab", first_fit, second_fit, preferred_element_type=jnp.float32)
    first_slot = pair_first[0, 0]
    live = pair_live[0, 0].astype(jnp.float32)
    first_orb = jnp.take(lax.dynamic_index_in_dim(first_in, d, 0, keepdims=False), jnp.arange(slots)) + c * occ
    own_second = lax.dynamic_index_in_dim(
        lax.dynamic_index_in_dim(pair_second, c, 0, keepdims=False), d, 0, keepdims=False)
    second_orb = own_second + jnp.arange(slots, dtype=jnp.int32) // per * occ
    denominator = (
        virt_energy[None, :, None]
        + virt_energy[None, None, :]
        - occ_energy[first_orb][:, None, None]
        - occ_energy[second_orb][:, None, None]
    )
    amplitude = (live[:, None, None] * intersection / denominator).astype(jnp.bfloat16)
    contribution = jnp.einsum("sab,sqb->sqa", amplitude, second_fit, preferred_element_type=jnp.float32)
    same = first_slot[:, None] == first_slot[None, :]
    gamma = []
    for s in range(slots):
        total = contribution[s]
        for t in range(slots):
            if t != s:
                total = total + jnp.where(same[s, t], contribution[t], 0.0)
        gamma.append(total.astype(jnp.bfloat16))
    gamma = jnp.stack(gamma)

    back = pl.pallas_call(
        functools.partial(return_kernel, orb, clu, xs),
        out_shape=jax.ShapeDtypeStruct((orb, slots, xs, virt), jnp.bfloat16),
        in_specs=[any_space],
        out_specs=any_space,
        scratch_shapes=[dma((orb,)), dma((orb,)), dma((1,))],
        compiler_params=pltpu.CompilerParams(collective_id=1, has_side_effects=True),
    )(gamma)

    earlier = (all_first[:, :, None] == all_first[:, None, :]) & (
        jnp.arange(slots)[None, :, None] > jnp.arange(slots)[None, None, :])
    speaks = ~jnp.any(earlier, axis=2)
    place = (
        (jnp.arange(occ, dtype=jnp.int32)[:, None] == first_in.reshape(-1)[None, :]) & speaks.reshape(-1)[None, :]
    ).astype(jnp.bfloat16)
    back = back.reshape(orb * slots, xs, virt).transpose(1, 0, 2)
    return jnp.einsum("oj,qja->qoa", place, back, preferred_element_type=jnp.float32).astype(jnp.bfloat16)


def solution(mesh):
    in_specs = (
        P("orb", "clu", None),
        P(None, "orb"),
        P(),
        P(),
        P(),
        P("clu", "orb", None),
        P(),
        P("clu", "orb", None),
    )
    out_specs = P("orb", "clu", None)
    return jax.shard_map(
        on_device, mesh=mesh, in_specs=in_specs, out_specs=out_specs, check_vma=False
    )
```
